16 devices in a mesh: dp: 2 (over y, z), ep: 8 (over x, core).
Axes of the slice: x: 4, y: 2, z: 1, core: 2. Of those that a mesh axis runs over, the one named last changes fastest.
The devices are a block of a 4x4x8 slice.
Arguments:
- hidden: bfloat16 [3072, 2560], P(('dp', 'ep')), parts along dimension 0
- route_idx: int32 [3072, 6], P(('dp', 'ep')), parts along dimension 0
- gate_weights: float32 [3072, 6], P(('dp', 'ep')), parts along dimension 0
- w_gate: bfloat16 [64, 2560, 1536], P('ep')
- w_up: bfloat16 [64, 2560, 1536], P('ep')
- w_down: bfloat16 [64, 1536, 2560], P('ep')
Outputs:
- output: bfloat16 [3072, 2560], P(('dp', 'ep')), parts along dimension 0
There are 2 independent parts. The reference program is written for one: setup_inputs(seed, part) draws one part's arguments, and reference() takes and returns one part's arrays. A program takes and returns all parts, laid end to end along the dimension named above; an argument that names none is the same for every part.
All inputs are finite; a program needn't handle non-finite values.
Results may differ from the reference program's by a relative error of at most 0.00119.
Values are sent between devices in bfloat16 or wider.
A program may use at most 768 MiB of HBM per device.

```python
import jax
import jax.numpy as jnp
from jax import lax

D_MODEL = 2560
D_FF = 1536
EXPERTS = 64
TOP_K = 6
GROUP_SIZE = 8
TOKENS_DEV = 192
ROW_CAP = 72
HOT_EXPERTS = 4

COLD_EXPERTS = EXPERTS - HOT_EXPERTS
REST_SLOTS = TOKENS_DEV * TOP_K - HOT_EXPERTS * ROW_CAP
COLD_SPREAD = min(REST_SLOTS // COLD_EXPERTS - 1, ROW_CAP - (REST_SLOTS + COLD_EXPERTS - 1) // COLD_EXPERTS)
COLD_PAIRS = COLD_EXPERTS // 2
TOKENS_PART = GROUP_SIZE * TOKENS_DEV


def draw_routes(route_key):
    key_hot, key_src = jax.random.split(route_key)
    expert_order = jax.random.permutation(key_hot, EXPERTS)
    cold_pos = jnp.arange(COLD_EXPERTS)
    cold_base = (cold_pos + 1) * REST_SLOTS // COLD_EXPERTS - cold_pos * REST_SLOTS // COLD_EXPERTS
    hot_counts = jnp.full((HOT_EXPERTS,), ROW_CAP, jnp.int32)
    slot_seq = jnp.arange(TOKENS_DEV * TOP_K)

    def one_source(src_key):
        key_shift, key_cold, key_tok, key_rot = jax.random.split(src_key, 4)
        pair_shift = jax.random.randint(key_shift, (COLD_PAIRS,), 0, COLD_SPREAD + 1)
        count_delta = jnp.concatenate([jnp.stack([pair_shift, -pair_shift], axis=1).reshape(-1), jnp.zeros((COLD_EXPERTS - 2 * COLD_PAIRS,), jnp.int32)])
        cold_counts = (cold_base + count_delta)[jax.random.permutation(key_cold, COLD_EXPERTS)]
        block_ends = jnp.cumsum(jnp.concatenate([hot_counts, cold_counts]))
        seq_experts = expert_order[jnp.searchsorted(block_ends, slot_seq, side='right')]
        choice_table = seq_experts.reshape(TOP_K, TOKENS_DEV).T[jax.random.permutation(key_tok, TOKENS_DEV)]
        slot_shift = jax.random.randint(key_rot, (TOKENS_DEV, 1), 0, TOP_K)
        slot_cols = (jnp.arange(TOP_K)[None, :] + slot_shift) % TOP_K
        return jnp.take_along_axis(choice_table, slot_cols, axis=1)

    all_routes = jax.vmap(one_source)(jax.random.split(key_src, GROUP_SIZE))
    return all_routes.reshape(TOKENS_PART, TOP_K).astype(jnp.int32)


def setup_inputs(seed: int = 0, part: int = 0) -> dict:
    base_key = jax.random.key(seed)
    part_key = jax.random.fold_in(base_key, part)
    key_x, key_gate, key_route = jax.random.split(part_key, 3)
    key_wg, key_wu, key_wd = jax.random.split(jax.random.key(seed + 1), 3)
    hidden = jax.random.normal(key_x, (TOKENS_PART, D_MODEL), jnp.float32).astype(jnp.bfloat16)
    gate_weights = jax.random.uniform(key_gate, (TOKENS_PART, TOP_K), jnp.float32, 0.3, 0.7) * (2.0 / TOP_K)
    route_idx = draw_routes(key_route)
    w_gate = (jax.random.normal(key_wg, (EXPERTS, D_MODEL, D_FF), jnp.float32) * D_MODEL ** -0.5).astype(jnp.bfloat16)
    w_up = (jax.random.normal(key_wu, (EXPERTS, D_MODEL, D_FF), jnp.float32) * D_MODEL ** -0.5).astype(jnp.bfloat16)
    w_down = (jax.random.normal(key_wd, (EXPERTS, D_FF, D_MODEL), jnp.float32) * (2.0 * D_FF ** -0.5)).astype(jnp.bfloat16)
    return {'hidden': hidden, 'route_idx': route_idx, 'gate_weights': gate_weights, 'w_gate': w_gate, 'w_up': w_up, 'w_down': w_down}


def reference(hidden, route_idx, gate_weights, w_gate, w_up, w_down):
    expert_cap = GROUP_SIZE * ROW_CAP
    pair_count = TOKENS_PART * TOP_K
    flat_ids = route_idx.reshape(-1)
    sort_order = jnp.argsort(flat_ids, stable=True)
    counts = jnp.bincount(flat_ids, length=EXPERTS)
    starts = jnp.cumsum(counts) - counts
    slot_range = jnp.arange(expert_cap)
    pair_pos = jnp.minimum(starts[:, None] + slot_range[None, :], pair_count - 1)
    pair_ids = sort_order[pair_pos]
    is_valid = slot_range[None, :] < counts[:, None]
    tok_rows = pair_ids // TOP_K
    row_gates = jnp.where(is_valid, gate_weights.reshape(-1)[pair_ids], 0.0)

    def expert_step(y_accum, scan_items):
        tok_idx, gate_col, gate_mat, up_mat, down_mat = scan_items
        expert_in = hidden[tok_idx]
        gate_proj = jnp.dot(expert_in, gate_mat, preferred_element_type=jnp.float32)
        up_proj = jnp.dot(expert_in, up_mat, preferred_element_type=jnp.float32)
        hidden_act = (jax.nn.silu(gate_proj) * up_proj).astype(jnp.bfloat16)
        expert_out = jnp.dot(hidden_act, down_mat, preferred_element_type=jnp.float32).astype(jnp.bfloat16)
        y_accum = y_accum.at[tok_idx].add(gate_col[:, None] * expert_out.astype(jnp.float32))
        return y_accum, None

    y_total = lax.scan(expert_step, jnp.zeros((TOKENS_PART, D_MODEL), jnp.float32), (tok_rows, row_gates, w_gate, w_up, w_down))[0]
    return y_total.astype(jnp.bfloat16)
```

```python
import functools

import jax
import jax.numpy as jnp
from jax import lax
from jax.experimental import pallas as pl
from jax.experimental.pallas import tpu as pltpu
from jax.sharding import PartitionSpec as P

MESH = pl.DeviceIdType.MESH
BF16 = jnp.bfloat16
F32 = jnp.float32
COL = 256
FCOL = 512
CHUNK = 16
W_SLOTS = 4
D_SLOTS = 8
VMEM_LIMIT = 63_000_000


def ring_places():
    me = lax.axis_index('ep')
    chip = me // 2
    core = lax.rem(me, 2)
    right = lax.rem(chip + 1, 4)
    far = lax.rem(chip + 2, 4)
    left = lax.rem(chip + 3, 4)
    return me, chip, core, right, left, far


def remote(src, dst, send_sem, recv_sem, device):
    return pltpu.make_async_remote_copy(src_ref=src, dst_ref=dst, send_sem=send_sem, recv_sem=recv_sem,
                                        device_id={'ep': device}, device_id_type=MESH)


def dispatch_kernel(tok, cap, win, x_hbm, meta_ref, xs_hbm, c_hbm, cnt_ref,
                    xbuf, mbuf, gbuf, stage, cstage, upper,
                    local_sem, meta_send, meta_recv, plus_send, plus_recv, minus_send, minus_recv,
                    pair_send, pair_recv, xs_sem, c_sem):
    me, chip, core, right, left, far = ring_places()
    n_dev = xbuf.shape[0]
    local_experts, _, pair_rows, d_model = xs_hbm.shape
    tiles = d_model // COL
    half = tiles // 2
    partner = chip * 2 + 1 - core
    right_dev, left_dev = right * 2 + core, left * 2 + core

    own_copy = pltpu.make_async_copy(x_hbm, xbuf.at[me], local_sem.at[0])
    own_copy.start()
    meta_copy = pltpu.make_async_copy(meta_ref, mbuf.at[me], local_sem.at[1])
    meta_copy.start()

    barrier = pltpu.get_barrier_semaphore()
    for k in range(1, n_dev):
        pl.semaphore_signal(barrier, inc=1, device_id={'ep': lax.rem(me + k, n_dev)}, device_id_type=MESH)
    pl.semaphore_wait(barrier, n_dev - 1)

    meta_copy.wait()
    for k in range(1, n_dev):
        remote(mbuf.at[me], mbuf.at[me], meta_send.at[k], meta_recv.at[k], lax.rem(me + k, n_dev)).start()
    own_copy.wait()

    def cols(j):
        return pl.ds(pl.multiple_of(j * COL, COL), COL)

    def block(dev, j):
        return xbuf.at[dev, :, cols(j)]

    def plus(j, slot, dev):
        return remote(block(dev, j), block(dev, j), plus_send.at[slot], plus_recv.at[slot], right_dev)

    def minus(j, slot, dev):
        return remote(block(dev, j), block(dev, j), minus_send.at[slot], minus_recv.at[slot], left_dev)

    def pair(j, group, dev):
        slot = group * tiles + j
        return remote(block(dev, j), block(dev, j), pair_send.at[slot], pair_recv.at[slot], partner)

    def send_own(j, _):
        plus(j, j, me).start()
        other = lax.rem(j + half, tiles)
        minus(other, other, me).start()
        pair(j, 0, me).start()
        return _

    lax.fori_loop(0, tiles, send_own, 0)

    row_i = lax.broadcasted_iota(jnp.int32, upper.shape, 0)
    col_i = lax.broadcasted_iota(jnp.int32, upper.shape, 1)
    same = (row_i < tok) == (col_i < tok)
    upper[...] = jnp.where((row_i < col_i) & same, 1.0, 0.0).astype(BF16)

    for k in range(1, n_dev):
        remote(mbuf.at[me], mbuf.at[lax.rem(me + n_dev - k, n_dev)], meta_send.at[k], meta_recv.at[k], partner).wait_recv()

    def plan(q, counts):
        meta = mbuf[2 * q] + mbuf[2 * q + 1]
        both = meta.shape[1]
        target = (lax.broadcasted_iota(jnp.int32, (local_experts, both), 0) + (me * local_experts + 1)).astype(F32)
        chosen = jnp.zeros((local_experts, both), F32)
        gates = jnp.zeros((local_experts, both), F32)
        for k in range(8):
            hit = jnp.broadcast_to(meta[k:k + 1, :], (local_experts, both)) == target
            chosen = jnp.where(hit, 1.0, chosen)
            gates = jnp.where(hit, jnp.broadcast_to(meta[8 + k:9 + k, :], (local_experts, both)), gates)
        rank = jnp.dot(chosen.astype(BF16), upper[...], preferred_element_type=F32)
        lane = lax.broadcasted_iota(jnp.int32, (local_experts, both), 1)
        first = lane < tok
        place = jnp.where(first, (cap - 1) - rank, cap + rank)
        place = jnp.where(chosen > 0, place, -4096.0)
        count0 = jnp.sum(jnp.where(first, chosen, 0.0), axis=1, keepdims=True)
        count1 = jnp.sum(jnp.where(first, 0.0, chosen), axis=1, keepdims=True)
        out_lane = lax.broadcasted_iota(jnp.int32, counts.shape, 1)
        counts = jnp.where(out_lane == 2 * q, count0, counts)
        counts = jnp.where(out_lane == 2 * q + 1, count1, counts)

        slot_i = lax.broadcasted_iota(jnp.int32, (pair_rows, both), 0).astype(F32)
        for e in range(local_experts):
            gbuf[q, e * pair_rows:(e + 1) * pair_rows, :] = jnp.where(slot_i == place[e:e + 1, :], 1.0, 0.0).astype(BF16)

        turned = jnp.concatenate([place, gates, jnp.zeros((128 - 2 * local_experts, both), F32)], axis=0).T
        for side in range(2):
            part = turned[side * tok:(side + 1) * tok, :]
            offset = 0 if side == 0 else pair_rows - win
            for lt in range(local_experts * win // 128):
                lanes = (lax.broadcasted_iota(jnp.int32, (tok, 128), 1) + lt * 128).astype(F32)
                acc = jnp.zeros((tok, 128), F32)
                for e in range(local_experts):
                    if e * win < (lt + 1) * 128 and (e + 1) * win > lt * 128:
                        acc = jnp.where(lanes == part[:, e:e + 1] + float(e * win - offset),
                                        part[:, local_experts + e:local_experts + e + 1], acc)
                hi = acc.astype(BF16)
                rest = acc - hi.astype(F32)
                mid = rest.astype(BF16)
                low = (rest - mid.astype(F32)).astype(BF16)
                where = slice(lt * 128, (lt + 1) * 128)
                cstage[2 * q + side, 0:tok, where] = hi
                cstage[2 * q + side, tok:2 * tok, where] = mid
                cstage[2 * q + side, 2 * tok:3 * tok, where] = low
        return counts

    counts = lax.fori_loop(0, n_dev // 2, plan, jnp.zeros(cnt_ref.shape, F32))
    cnt_ref[...] = counts.astype(jnp.int32)
    c_copy = pltpu.make_async_copy(cstage, c_hbm, c_sem)
    c_copy.start()

    def xs_copy(q, j):
        return pltpu.make_async_copy(stage.at[q, :, :, cols(j)], xs_hbm.at[:, q, :, cols(j)], xs_sem.at[q, j])

    def pick(q, j):
        rows = xbuf[pl.ds(2 * q, 2), :, cols(j)].reshape(2 * tok, COL)
        hold = local_experts // 2
        for part in range(2):
            sel = gbuf[q, part * hold * pair_rows:(part + 1) * hold * pair_rows, :]
            got = jnp.dot(sel, rows, preferred_element_type=F32).astype(BF16)
            stage[q, part * hold:(part + 1) * hold, :, cols(j)] = got.reshape(hold, pair_rows, COL)
        xs_copy(q, j).start()

    def pick_own(j, _):
        pair(j, 0, partner).wait_recv()
        pick(chip, j)
        return _

    lax.fori_loop(0, tiles, pick_own, 0)

    def near_a(i, _):
        plus(i, i, left_dev).wait_recv()
        plus(i, tiles + i, left_dev).start()
        pair(i, 1, left_dev).start()
        j = half + i
        minus(j, j, right_dev).wait_recv()
        minus(j, tiles + i, right_dev).start()
        pair(j, 2, right_dev).start()
        return _

    lax.fori_loop(0, half, near_a, 0)

    left_other, right_other = left * 2 + 1 - core, right * 2 + 1 - core

    def near_b(i, _):
        j = half + i
        plus(j, j, left_dev).wait_recv()
        pair(j, 1, left_dev).start()
        minus(i, i, right_dev).wait_recv()
        pair(i, 2, right_dev).start()
        pair(i, 1, left_other).wait_recv()
        pick(left, i)
        pair(j, 2, right_other).wait_recv()
        pick(right, j)
        return _

    lax.fori_loop(0, half, near_b, 0)

    far_dev, far_other = far * 2 + core, far * 2 + 1 - core

    def far_c(i, _):
        j = half + i
        plus(i, tiles + i, far_dev).wait_recv()
        pair(i, 3, far_dev).start()
        minus(j, tiles + i, far_dev).wait_recv()
        pair(j, 3, far_dev).start()
        pair(j, 1, left_other).wait_recv()
        pick(left, j)
        pair(i, 2, right_other).wait_recv()
        pick(right, i)
        return _

    lax.fori_loop(0, half, far_c, 0)

    def far_d(i, _):
        j = half + i
        pair(i, 3, far_other).wait_recv()
        pick(far, i)
        pair(j, 3, far_other).wait_recv()
        pick(far, j)
        return _

    lax.fori_loop(0, half, far_d, 0)

    for k in range(1, n_dev):
        remote(mbuf.at[me], mbuf.at[me], meta_send.at[k], meta_recv.at[k], partner).wait_send()

    def drain_ring(s, _):
        plus(0, s, me).wait_send()
        minus(0, s, me).wait_send()
        return _

    lax.fori_loop(0, tiles + half, drain_ring, 0)

    def drain_pair(s, _):
        for group in range(4):
            pair(s, group, me).wait_send()
        for q in range(n_dev // 2):
            xs_copy(q, s).wait()
        return _

    lax.fori_loop(0, tiles, drain_pair, 0)
    c_copy.wait()


def ffn_kernel(cap, cnt_ref, xs_hbm, wg_hbm, wu_hbm, h_hbm, xbuf, gbuf, ubuf, hbuf, zbuf, x_sem, w_sem, h_sem):
    experts, chips, pair_rows, _ = xs_hbm.shape
    d_ff = h_hbm.shape[3]
    f_tiles = d_ff // FCOL
    steps = experts * f_tiles
    per_chip = pair_rows // CHUNK
    all_rows = chips * pair_rows
    zbuf[...] = jnp.zeros_like(zbuf)

    def chunk_range(e, p):
        lo = (cap - cnt_ref[e, 2 * p]) // CHUNK
        hi = (cap + cnt_ref[e, 2 * p + 1] + (CHUNK - 1)) // CHUNK
        return lo, hi

    def chunk(i):
        return pl.ds(pl.multiple_of(i * CHUNK, CHUNK), CHUNK)

    def chunk_total(e):
        total = jnp.int32(0)
        for p in range(chips):
            lo, hi = chunk_range(e, p)
            total = total + (hi - lo)
        return total

    def x_copy(e, p, j, slot, i):
        return pltpu.make_async_copy(xs_hbm.at[e, p, chunk(j), :], xbuf.at[slot, chunk(i), :], x_sem.at[slot, i])

    def start_x(e, slot):
        base = jnp.int32(0)
        for p in range(chips):
            lo, hi = chunk_range(e, p)

            def one(j, _, p=p, lo=lo, base=base):
                x_copy(e, p, j, slot, base + j - lo).start()
                return _

            lax.fori_loop(lo, hi, one, 0)
            base = base + (hi - lo)

    def w_copies(step):
        e, f, slot = step // f_tiles, lax.rem(step, f_tiles), lax.rem(step, W_SLOTS)
        where = pl.ds(pl.multiple_of(f * FCOL, FCOL), FCOL)
        return (pltpu.make_async_copy(wg_hbm.at[e, :, where], gbuf.at[slot], w_sem.at[slot, 0]),
                pltpu.make_async_copy(wu_hbm.at[e, :, where], ubuf.at[slot], w_sem.at[slot, 1]))

    def start_w(step):
        for copy in w_copies(step):
            copy.start()

    def start_h(e, slot):
        base = jnp.int32(0)
        for p in range(chips):
            lo, hi = chunk_range(e, p)

            def one(j, _, p=p, lo=lo, hi=hi, base=base):
                live = (j >= lo) & (j < hi)

                @pl.when(live)
                def _live():
                    pltpu.make_async_copy(hbuf.at[slot, chunk(base + j - lo), :], h_hbm.at[e, p, chunk(j), :],
                                          h_sem.at[slot, p, j]).start()

                @pl.when(jnp.logical_not(live))
                def _dead():
                    pltpu.make_async_copy(zbuf, h_hbm.at[e, p, chunk(j), :], h_sem.at[slot, p, j]).start()

                return _

            lax.fori_loop(0, per_chip, one, 0)
            base = base + (hi - lo)

    def wait_h(slot):
        for p in range(chips):

            def one(j, _, p=p):
                pltpu.make_async_copy(zbuf, h_hbm.at[0, p, chunk(j), :], h_sem.at[slot, p, j]).wait()
                return _

            lax.fori_loop(0, per_chip, one, 0)

    for s in range(min(W_SLOTS, steps)):
        start_w(jnp.int32(s))
        if s == 0:
            start_x(jnp.int32(0), 0)

    sizes = sorted({min(all_rows, m) for m in (128, 192, 256, 384, all_rows)})

    def body(step, _):
        e, f, slot = step // f_tiles, lax.rem(step, f_tiles), lax.rem(step, W_SLOTS)
        side = lax.rem(e, 2)
        total = chunk_total(e)

        @pl.when(f == 0)
        def _enter():
            @pl.when(e + 1 < experts)
            def _next():
                start_x(e + 1, 1 - side)

            def one(i, _):
                x_copy(0, 0, 0, side, i).wait()
                return _

            lax.fori_loop(0, total, one, 0)

            @pl.when(e >= 2)
            def _reuse():
                wait_h(side)

        for copy in w_copies(step):
            copy.wait()
        where = pl.ds(pl.multiple_of(f * FCOL, FCOL), FCOL)
        below = 0
        for size in sizes:
            @pl.when((total > below) & (total <= size // CHUNK))
            def _run(size=size):
                rows = xbuf[side, 0:size, :]
                gate = jnp.dot(rows, gbuf[slot], preferred_element_type=F32)
                up = jnp.dot(rows, ubuf[slot], preferred_element_type=F32)
                hbuf[side, 0:size, where] = (jax.nn.silu(gate) * up).astype(BF16)

            below = size // CHUNK

        @pl.when(step + W_SLOTS < steps)
        def _more():
            start_w(step + W_SLOTS)

        @pl.when(f == f_tiles - 1)
        def _leave():
            start_h(e, side)

        return _

    lax.fori_loop(0, steps, body, 0)
    wait_h(0)
    wait_h(1)


def combine_kernel(tok, win, h_hbm, c_hbm, wd_hbm, out_ref,
                   hbuf, cbuf, wbuf, obuf, ysend, zbuf, pbuf, fbuf, nbuf,
                   h_sem, c_sem, w_sem, y_send, y_recv, far_send, far_recv, near_send, near_recv):
    me, chip, core, right, left, far = ring_places()
    experts, rows, _ = h_hbm.shape
    chips = 4
    pair_rows = rows // chips
    tiles = out_ref.shape[1] // COL
    steps = tiles * experts
    partner = chip * 2 + 1 - core
    right_dev, left_dev = right * 2 + core, left * 2 + core
    dests = (far, right, left, chip)
    cut = tok // 2

    def cols(j):
        return pl.ds(pl.multiple_of(j * COL, COL), COL)

    def w_copy(step):
        t, e, slot = step // experts, lax.rem(step, experts), lax.rem(step, D_SLOTS)
        return pltpu.make_async_copy(wd_hbm.at[e, :, cols(t)], wbuf.at[slot], w_sem.at[slot])

    def h_copy(e):
        return pltpu.make_async_copy(h_hbm.at[e], hbuf.at[e], h_sem.at[e])

    c_copy = pltpu.make_async_copy(c_hbm, cbuf, c_sem)
    for e in range(experts):
        h_copy(e).start()
        if e < D_SLOTS:
            w_copy(jnp.int32(e)).start()
    c_copy.start()

    barrier = pltpu.get_barrier_semaphore()
    for dev in (partner, right_dev, left_dev):
        pl.semaphore_signal(barrier, inc=1, device_id={'ep': dev}, device_id_type=MESH)
    pl.semaphore_wait(barrier, 3)

    def y_copy(t, d):
        return remote(ysend.at[lax.rem(t, 2), d], pbuf.at[t, d], y_send.at[lax.rem(t, 2), d], y_recv.at[t, d], partner)

    def far_copy(t, side):
        src = zbuf.at[lax.rem(t, 3), 0, pl.ds(side * cut, cut), :]
        return remote(src, fbuf.at[t, side], far_send.at[t, side], far_recv.at[t, side], (right_dev, left_dev)[side])

    def near_copy(t, side):
        src = zbuf.at[lax.rem(t, 3), 1 + side]
        return remote(src, nbuf.at[t, side], near_send.at[t, side], near_recv.at[t, side], (right_dev, left_dev)[side])

    def gated(s):
        three = jnp.dot(cbuf[s], obuf[s], preferred_element_type=F32)
        return three[0:tok] + three[tok:2 * tok] + three[2 * tok:3 * tok]

    def project(t):
        def one(e, _):
            step = t * experts + e

            @pl.when(t == 0)
            def _first():
                pltpu.make_async_copy(h_hbm.at[e], hbuf.at[e], h_sem.at[e]).wait()

            w_copy(step).wait()
            o = jnp.dot(hbuf[e], wbuf[lax.rem(step, D_SLOTS)], preferred_element_type=F32).astype(BF16)
            here = pl.ds(pl.multiple_of(e * win, CHUNK), win)
            for p in range(chips):
                obuf[2 * p, here, :] = o[p * pair_rows:p * pair_rows + win]
                obuf[2 * p + 1, here, :] = o[(p + 1) * pair_rows - win:(p + 1) * pair_rows]

            @pl.when(step + D_SLOTS < steps)
            def _more():
                w_copy(step + D_SLOTS).start()

            return _

        lax.fori_loop(0, experts, one, 0)

    def pass_on(t):
        for side in range(2):
            far_copy(t, side).wait_recv()
            part = pl.ds(side * cut, cut)
            zbuf[lax.rem(t, 3), 1 + side, part, :] += fbuf[t, side]
            near_copy(t, side).start()

    def sums(t):
        @pl.when(t >= 2)
        def _reuse():
            for d in range(4):
                y_copy(t - 2, d).wait_send()

        for d in range(4):
            ysend[lax.rem(t, 2), d] = gated(2 * dests[d] + 1 - core)
            y_copy(t, d).start()
        for d in range(4):
            own = gated(2 * dests[d] + core)
            y_copy(t, d).wait_recv()
            zbuf[lax.rem(t, 3), d] = own + pbuf[t, d]
            if d == 0:
                far_copy(t, 0).start()
                far_copy(t, 1).start()

    def finish(t):
        near_copy(t, 0).wait_recv()
        near_copy(t, 1).wait_recv()
        total = zbuf[lax.rem(t, 3), 3] + nbuf[t, 0] + nbuf[t, 1]
        out_ref[:, cols(t)] = total.astype(out_ref.dtype)
        for side in range(2):
            far_copy(t, side).wait_send()
            near_copy(t, side).wait_send()

    def body(t, _):
        @pl.when(t < tiles)
        def _project():
            project(t)

        @pl.when(t == 0)
        def _gates():
            c_copy.wait()

        @pl.when((t >= 1) & (t <= tiles))
        def _pass_on():
            pass_on(t - 1)

        @pl.when(t >= 2)
        def _finish():
            finish(t - 2)

        @pl.when(t < tiles)
        def _sums():
            sums(t)

        return _

    lax.fori_loop(0, tiles + 2, body, 0)
    for back in (2, 1):
        for d in range(4):
            y_copy(jnp.int32(tiles - back), d).wait_send()


def solution(mesh):
    ep_size = mesh.shape['ep']
    chips = ep_size // 2

    def device_body(hidden, route_idx, gate_weights, w_gate, w_up, w_down):
        tok, top_k = route_idx.shape
        d_model = hidden.shape[1]
        experts, _, d_ff = w_gate.shape
        num_experts = experts * ep_size
        cap = min(tok, 4 * top_k * tok // num_experts)
        pair_rows = 2 * cap
        win = (cap + CHUNK - 1) // CHUNK * CHUNK
        tiles = d_model // COL
        rows = chips * pair_rows
        any_space = pl.BlockSpec(memory_space=pl.ANY)
        vmem = pl.BlockSpec(memory_space=pltpu.VMEM)
        dma = pltpu.SemaphoreType.DMA

        core = lax.rem(lax.axis_index('ep'), 2)
        packed = jnp.zeros((2, 8, tok), F32)
        packed = packed.at[0, :top_k].set(route_idx.T.astype(F32) + 1.0).at[1, :top_k].set(gate_weights.T)
        packed = packed.reshape(16, tok)
        blank = jnp.zeros_like(packed)
        meta = jnp.concatenate([jnp.where(core == 0, packed, blank), jnp.where(core == 1, packed, blank)], axis=1)

        xs, gates, counts = pl.pallas_call(
            functools.partial(dispatch_kernel, tok, cap, win),
            out_shape=(jax.ShapeDtypeStruct((experts, chips, pair_rows, d_model), BF16),
                       jax.ShapeDtypeStruct((ep_size, 3 * tok, experts * win), BF16),
                       jax.ShapeDtypeStruct((experts, 128), jnp.int32)),
            in_specs=[any_space, vmem],
            out_specs=(any_space, any_space, vmem),
            scratch_shapes=[
                pltpu.VMEM((ep_size, tok, d_model), BF16),
                pltpu.VMEM((ep_size, 16, 2 * tok), F32),
                pltpu.VMEM((chips, experts * pair_rows, 2 * tok), BF16),
                pltpu.VMEM((chips, experts, pair_rows, d_model), BF16),
                pltpu.VMEM((ep_size, 3 * tok, experts * win), BF16),
                pltpu.VMEM((2 * tok, 2 * tok), BF16),
                dma((2,)), dma((ep_size,)), dma((ep_size,)),
                dma((tiles + tiles // 2,)), dma((tiles + tiles // 2,)), dma((tiles + tiles // 2,)), dma((tiles + tiles // 2,)),
                dma((4 * tiles,)), dma((4 * tiles,)), dma((chips, tiles)), dma,
            ],
            compiler_params=pltpu.CompilerParams(collective_id=0, has_side_effects=True, vmem_limit_bytes=VMEM_LIMIT),
            name='dispatch',
        )(hidden, meta)

        act = pl.pallas_call(
            functools.partial(ffn_kernel, cap),
            out_shape=jax.ShapeDtypeStruct((experts, chips, pair_rows, d_ff), BF16),
            in_specs=[pl.BlockSpec(memory_space=pltpu.SMEM), any_space, any_space, any_space],
            out_specs=any_space,
            scratch_shapes=[
                pltpu.VMEM((2, rows, d_model), BF16),
                pltpu.VMEM((W_SLOTS, d_model, FCOL), BF16),
                pltpu.VMEM((W_SLOTS, d_model, FCOL), BF16),
                pltpu.VMEM((2, rows, d_ff), BF16),
                pltpu.VMEM((CHUNK, d_ff), BF16),
                dma((2, rows // CHUNK)), dma((W_SLOTS, 2)), dma((2, chips, pair_rows // CHUNK)),
            ],
            compiler_params=pltpu.CompilerParams(vmem_limit_bytes=VMEM_LIMIT),
            name='gate_up',
        )(counts, xs, w_gate, w_up)

        return pl.pallas_call(
            functools.partial(combine_kernel, tok, win),
            out_shape=jax.ShapeDtypeStruct((tok, d_model), BF16),
            in_specs=[any_space, any_space, any_space],
            out_specs=vmem,
            scratch_shapes=[
                pltpu.VMEM((experts, rows, d_ff), BF16),
                pltpu.VMEM((ep_size, 3 * tok, experts * win), BF16),
                pltpu.VMEM((D_SLOTS, d_ff, COL), BF16),
                pltpu.VMEM((ep_size, experts * win, COL), BF16),
                pltpu.VMEM((2, chips, tok, COL), F32),
                pltpu.VMEM((3, chips, tok, COL), F32),
                pltpu.VMEM((tiles, chips, tok, COL), F32),
                pltpu.VMEM((tiles, 2, tok // 2, COL), F32),
                pltpu.VMEM((tiles, 2, tok, COL), F32),
                dma((experts,)), dma, dma((D_SLOTS,)),
                dma((2, chips)), dma((tiles, chips)), dma((tiles, 2)), dma((tiles, 2)), dma((tiles, 2)), dma((tiles, 2)),
            ],
            compiler_params=pltpu.CompilerParams(collective_id=1, has_side_effects=True, vmem_limit_bytes=VMEM_LIMIT),
            name='down_combine',
        )(act.reshape(experts, rows, d_ff), gates, w_down)

    row_spec = P(('dp', 'ep'), None)
    expert_spec = P('ep', None, None)
    return jax.shard_map(device_body, mesh=mesh, in_specs=(row_spec, row_spec, row_spec, expert_spec, expert_spec, expert_spec), out_specs=row_spec, check_vma=False)
```

```python
import functools

import jax
import jax.numpy as jnp
from jax import lax
from jax.experimental import pallas as pl
from jax.experimental.pallas import tpu as pltpu
from jax.sharding import PartitionSpec as P

MESH = pl.DeviceIdType.MESH
BF16 = jnp.bfloat16
F32 = jnp.float32
COL = 256
WIDE = 512
FCOL = 512
CHUNK = 16
W_SLOTS = 4
DN_SLOTS = 6
D_SLOTS = 6
EARLY = 3
Z_SLOTS = 3
VMEM_LIMIT = 63_000_000


def ring_places():
    me = lax.axis_index('ep')
    chip = me // 2
    core = lax.rem(me, 2)
    right = lax.rem(chip + 1, 4)
    far = lax.rem(chip + 2, 4)
    left = lax.rem(chip + 3, 4)
    return me, chip, core, right, left, far


def remote(src, dst, send_sem, recv_sem, device):
    return pltpu.make_async_remote_copy(src_ref=src, dst_ref=dst, send_sem=send_sem, recv_sem=recv_sem,
                                        device_id={'ep': device}, device_id_type=MESH)


def dispatch_kernel(tok, cap, win, x_hbm, meta_ref, xs_hbm, c_hbm, cnt_ref,
                    xbuf, mbuf, gbuf, stage, cstage, upper,
                    local_sem, meta_send, meta_recv, plus_send, plus_recv, minus_send, minus_recv,
                    pair_send, pair_recv, xs_sem, c_sem):
    me, chip, core, right, left, far = ring_places()
    n_dev = xbuf.shape[0]
    local_experts, _, pair_rows, d_model = xs_hbm.shape
    tiles = d_model // COL
    half = tiles // 2
    partner = chip * 2 + 1 - core
    right_dev, left_dev = right * 2 + core, left * 2 + core

    own_copy = pltpu.make_async_copy(x_hbm, xbuf.at[me], local_sem.at[0])
    own_copy.start()
    meta_copy = pltpu.make_async_copy(meta_ref, mbuf.at[me], local_sem.at[1])
    meta_copy.start()

    far_same = far * 2 + core
    barrier = pltpu.get_barrier_semaphore()
    for dev in (partner, right_dev, left_dev, far_same):
        pl.semaphore_signal(barrier, inc=1, device_id={'ep': dev}, device_id_type=MESH)
    pl.semaphore_wait(barrier, 4)

    def meta_send_to(slot, source, device):
        return remote(mbuf.at[source], mbuf.at[source], meta_send.at[slot], meta_recv.at[slot], device)

    meta_copy.wait()
    for slot, dev in enumerate((right_dev, left_dev, far_same, partner)):
        meta_send_to(slot, me, dev).start()
    own_copy.wait()

    def cols(j):
        return pl.ds(pl.multiple_of(j * COL, COL), COL)

    def block(dev, j):
        return xbuf.at[dev, :, cols(j)]

    def plus(j, slot, dev):
        return remote(block(dev, j), block(dev, j), plus_send.at[slot], plus_recv.at[slot], right_dev)

    def minus(j, slot, dev):
        return remote(block(dev, j), block(dev, j), minus_send.at[slot], minus_recv.at[slot], left_dev)

    def pair(j, group, dev):
        slot = group * tiles + j
        return remote(block(dev, j), block(dev, j), pair_send.at[slot], pair_recv.at[slot], partner)

    def send_own(j, _):
        plus(j, j, me).start()
        other = lax.rem(j + half, tiles)
        minus(other, other, me).start()
        pair(j, 0, me).start()
        return _

    lax.fori_loop(0, tiles, send_own, 0)

    row_i = lax.broadcasted_iota(jnp.int32, upper.shape, 0)
    col_i = lax.broadcasted_iota(jnp.int32, upper.shape, 1)
    same = (row_i < tok) == (col_i < tok)
    upper[...] = jnp.where((row_i < col_i) & same, 1.0, 0.0).astype(BF16)

    for slot, dev in enumerate((left_dev, right_dev, far_same)):
        meta_send_to(slot, dev, partner).wait_recv()
        meta_send_to(4 + slot, dev, partner).start()
    for slot, q in ((3, chip), (4, left), (5, right), (6, far)):
        meta_send_to(slot, 2 * q + 1 - core, partner).wait_recv()

    def plan(q, counts):
        one, two = mbuf[2 * q], mbuf[2 * q + 1]
        both = one.shape[1]
        low = lax.broadcasted_iota(jnp.int32, one.shape, 1) < tok
        ids = jnp.where(low, one, pltpu.roll(two, tok, 1))
        weights = jnp.where(low, pltpu.roll(one, tok, 1), two)
        target = (lax.broadcasted_iota(jnp.int32, (local_experts, both), 0) + (me * local_experts + 1)).astype(F32)
        chosen = jnp.zeros((local_experts, both), F32)
        gates = jnp.zeros((local_experts, both), F32)
        for k in range(ids.shape[0]):
            hit = jnp.broadcast_to(ids[k:k + 1, :], (local_experts, both)) == target
            chosen = jnp.where(hit, 1.0, chosen)
            gates = jnp.where(hit, jnp.broadcast_to(weights[k:k + 1, :], (local_experts, both)), gates)
        rank = jnp.dot(chosen.astype(BF16), upper[...], preferred_element_type=F32)
        lane = lax.broadcasted_iota(jnp.int32, (local_experts, both), 1)
        first = lane < tok
        place = jnp.where(first, (cap - 1) - rank, cap + rank)
        place = jnp.where(chosen > 0, place, -4096.0)
        count0 = jnp.sum(jnp.where(first, chosen, 0.0), axis=1, keepdims=True)
        count1 = jnp.sum(jnp.where(first, 0.0, chosen), axis=1, keepdims=True)
        out_lane = lax.broadcasted_iota(jnp.int32, counts.shape, 1)
        counts = jnp.where(out_lane == 2 * q, count0, counts)
        counts = jnp.where(out_lane == 2 * q + 1, count1, counts)

        slot_i = lax.broadcasted_iota(jnp.int32, (pair_rows, both), 0).astype(F32)
        for e in range(local_experts):
            gbuf[q, e * pair_rows:(e + 1) * pair_rows, :] = jnp.where(slot_i == place[e:e + 1, :], 1.0, 0.0).astype(BF16)

        turned = jnp.concatenate([place, gates, jnp.zeros((128 - 2 * local_experts, both), F32)], axis=0).T
        for side in range(2):
            part = turned[side * tok:(side + 1) * tok, :]
            offset = 0 if side == 0 else pair_rows - win
            for lt in range(local_experts * win // 128):
                lanes = (lax.broadcasted_iota(jnp.int32, (tok, 128), 1) + lt * 128).astype(F32)
                acc = jnp.zeros((tok, 128), F32)
                for e in range(local_experts):
                    if e * win < (lt + 1) * 128 and (e + 1) * win > lt * 128:
                        acc = jnp.where(lanes == part[:, e:e + 1] + float(e * win - offset),
                                        part[:, local_experts + e:local_experts + e + 1], acc)
                hi = acc.astype(BF16)
                rest = acc - hi.astype(F32)
                mid = rest.astype(BF16)
                tail = (rest - mid.astype(F32)).astype(BF16)
                where = slice(lt * 128, (lt + 1) * 128)
                cstage[2 * q + side, 0:tok, where] = hi
                cstage[2 * q + side, tok:2 * tok, where] = mid
                cstage[2 * q + side, 2 * tok:3 * tok, where] = tail
        return counts

    counts = lax.fori_loop(0, n_dev // 2, plan, jnp.zeros(cnt_ref.shape, F32))
    cnt_ref[...] = counts.astype(jnp.int32)
    c_copy = pltpu.make_async_copy(cstage, c_hbm, c_sem)
    c_copy.start()

    def xs_copy(q, j):
        return pltpu.make_async_copy(stage.at[q, :, :, cols(j)], xs_hbm.at[:, q, :, cols(j)], xs_sem.at[q, j])

    def pick(q, j):
        rows = xbuf[pl.ds(2 * q, 2), :, cols(j)].reshape(2 * tok, COL)
        hold = local_experts // 2
        for part in range(2):
            sel = gbuf[q, part * hold * pair_rows:(part + 1) * hold * pair_rows, :]
            got = jnp.dot(sel, rows, preferred_element_type=F32).astype(BF16)
            stage[q, part * hold:(part + 1) * hold, :, cols(j)] = got.reshape(hold, pair_rows, COL)
        xs_copy(q, j).start()

    def pick_own(j, _):
        pair(j, 0, partner).wait_recv()
        pick(chip, j)
        return _

    lax.fori_loop(0, tiles, pick_own, 0)

    def near_a(i, _):
        plus(i, i, left_dev).wait_recv()
        plus(i, tiles + i, left_dev).start()
        pair(i, 1, left_dev).start()
        j = half + i
        minus(j, j, right_dev).wait_recv()
        minus(j, tiles + i, right_dev).start()
        pair(j, 2, right_dev).start()
        return _

    lax.fori_loop(0, half, near_a, 0)

    left_other, right_other = left * 2 + 1 - core, right * 2 + 1 - core

    def near_b(i, _):
        j = half + i
        plus(j, j, left_dev).wait_recv()
        pair(j, 1, left_dev).start()
        minus(i, i, right_dev).wait_recv()
        pair(i, 2, right_dev).start()
        pair(i, 1, left_other).wait_recv()
        pick(left, i)
        pair(j, 2, right_other).wait_recv()
        pick(right, j)

        @pl.when(i > 0)
        def _late():
            pair(j - 1, 1, left_other).wait_recv()
            pick(left, j - 1)
            pair(i - 1, 2, right_other).wait_recv()
            pick(right, i - 1)

        return _

    lax.fori_loop(0, half, near_b, 0)
    pair(tiles - 1, 1, left_other).wait_recv()
    pick(left, tiles - 1)
    pair(half - 1, 2, right_other).wait_recv()
    pick(right, half - 1)

    far_dev, far_other = far * 2 + core, far * 2 + 1 - core

    def far_c(i, _):
        @pl.when(i < half)
        def _arrive():
            plus(i, tiles + i, far_dev).wait_recv()
            pair(i, 3, far_dev).start()
            minus(half + i, tiles + i, far_dev).wait_recv()
            pair(half + i, 3, far_dev).start()

        @pl.when(i > 0)
        def _late():
            pair(i - 1, 3, far_other).wait_recv()
            pick(far, i - 1)
            pair(half + i - 1, 3, far_other).wait_recv()
            pick(far, half + i - 1)

        return _

    lax.fori_loop(0, half + 1, far_c, 0)

    for slot in range(7):
        meta_send_to(slot, me, partner).wait_send()

    def drain_ring(s, _):
        plus(0, s, me).wait_send()
        minus(0, s, me).wait_send()
        return _

    lax.fori_loop(0, tiles + half, drain_ring, 0)

    def drain_pair(s, _):
        for group in range(4):
            pair(s, group, me).wait_send()
        for q in range(n_dev // 2):
            xs_copy(q, s).wait()
        return _

    lax.fori_loop(0, tiles, drain_pair, 0)
    c_copy.wait()


def ffn_kernel(cap, early, cnt_ref, xs_hbm, wg_hbm, wu_hbm, wd_hbm, out_hbm, h_hbm,
               xbuf, gbuf, ubuf, dbuf, hbuf, zbuf, x_sem, w_sem, d_sem, h_sem):
    experts, chips, pair_rows, d_model = xs_hbm.shape
    d_ff = hbuf.shape[2]
    f_tiles, d_tiles = d_ff // FCOL, d_model // FCOL
    steps = experts * f_tiles
    d_steps = early * d_tiles
    per_chip = pair_rows // CHUNK
    all_rows = chips * pair_rows
    zbuf[...] = jnp.zeros_like(zbuf)

    def chunk_range(e, p):
        lo = (cap - cnt_ref[e, 2 * p]) // CHUNK
        hi = (cap + cnt_ref[e, 2 * p + 1] + (CHUNK - 1)) // CHUNK
        return lo, hi

    def chunk(i):
        return pl.ds(pl.multiple_of(i * CHUNK, CHUNK), CHUNK)

    def chunk_total(e):
        total = jnp.int32(0)
        for p in range(chips):
            lo, hi = chunk_range(e, p)
            total = total + (hi - lo)
        return total

    def each_chunk(e, act):
        base = jnp.int32(0)
        for p in range(chips):
            lo, hi = chunk_range(e, p)

            def one(j, _, p=p, lo=lo, base=base):
                act(p, j, base + j - lo)
                return _

            lax.fori_loop(lo, hi, one, 0)
            base = base + (hi - lo)

    def x_copy(e, p, j, slot, i):
        return pltpu.make_async_copy(xs_hbm.at[e, p, chunk(j), :], xbuf.at[slot, chunk(i), :], x_sem.at[slot, i])

    def o_copy(e, p, j, slot, i):
        return pltpu.make_async_copy(xbuf.at[slot, chunk(i), :], out_hbm.at[e, p, chunk(j), :], x_sem.at[slot, i])

    def wait_rows(e, slot, copy):
        def one(i, _):
            copy(0, 0, 0, slot, i).wait()
            return _

        lax.fori_loop(0, chunk_total(e), one, 0)

    def start_x(e):
        slot = lax.rem(e, 3)
        each_chunk(e, lambda p, j, i: x_copy(e, p, j, slot, i).start())

    def w_copies(step):
        e, f, slot = step // f_tiles, lax.rem(step, f_tiles), lax.rem(step, W_SLOTS)
        where = pl.ds(pl.multiple_of(f * FCOL, FCOL), FCOL)
        return (pltpu.make_async_copy(wg_hbm.at[e, :, where], gbuf.at[slot], w_sem.at[slot, 0]),
                pltpu.make_async_copy(wu_hbm.at[e, :, where], ubuf.at[slot], w_sem.at[slot, 1]))

    def start_w(step):
        for copy in w_copies(step):
            copy.start()

    def d_copy(step):
        e, f, slot = step // d_tiles, lax.rem(step, d_tiles), lax.rem(step, DN_SLOTS)
        where = pl.ds(pl.multiple_of(f * FCOL, FCOL), FCOL)
        return pltpu.make_async_copy(wd_hbm.at[e, :, where], dbuf.at[slot], d_sem.at[slot])

    def start_h(e, slot):
        base = jnp.int32(0)
        for p in range(chips):
            lo, hi = chunk_range(e, p)

            def one(j, _, p=p, lo=lo, hi=hi, base=base):
                live = (j >= lo) & (j < hi)

                @pl.when(live)
                def _live():
                    pltpu.make_async_copy(hbuf.at[slot, chunk(base + j - lo), :], h_hbm.at[e - early, p, chunk(j), :],
                                          h_sem.at[slot, p, j]).start()

                @pl.when(jnp.logical_not(live))
                def _dead():
                    pltpu.make_async_copy(zbuf, h_hbm.at[e - early, p, chunk(j), :], h_sem.at[slot, p, j]).start()

                return _

            lax.fori_loop(0, per_chip, one, 0)
            base = base + (hi - lo)

    def wait_h(slot):
        for p in range(chips):

            def one(j, _, p=p):
                pltpu.make_async_copy(zbuf, h_hbm.at[0, p, chunk(j), :], h_sem.at[slot, p, j]).wait()
                return _

            lax.fori_loop(0, per_chip, one, 0)

    start_x(jnp.int32(0))
    for s in range(min(W_SLOTS, steps)):
        start_w(jnp.int32(s))
        if s < min(DN_SLOTS, d_steps) and s < f_tiles:
            d_copy(jnp.int32(s)).start()
    for s in range(min(W_SLOTS, f_tiles), min(DN_SLOTS, d_steps)):
        d_copy(jnp.int32(s)).start()

    sizes = sorted({min(all_rows, m) for m in (128, 192, 256, 384, all_rows)})

    def sized(total, run):
        below = 0
        for size in sizes:
            @pl.when((total > below) & (total <= size // CHUNK))
            def _run(size=size):
                run(size)

            below = size // CHUNK

    def columns(f):
        return pl.ds(pl.multiple_of(f * FCOL, FCOL), FCOL)

    def expert(e, _):
        slot, side = lax.rem(e, 3), lax.rem(e, 2)
        total = chunk_total(e)

        @pl.when((e >= 2) & (e - 2 < early))
        def _sent():
            wait_rows(e - 2, lax.rem(e - 2, 3), lambda *a: o_copy(*a))

        @pl.when(e + 1 < experts)
        def _next():
            start_x(e + 1)

        wait_rows(e, slot, lambda *a: x_copy(*a))

        if early < experts:
            @pl.when(e - 2 >= early)
            def _reuse():
                wait_h(side)

        def gate_up(f, _):
            step = e * f_tiles + f
            ring = lax.rem(step, W_SLOTS)
            for copy in w_copies(step):
                copy.wait()

            def run(size):
                rows = xbuf[slot, 0:size, :]
                gate = jnp.dot(rows, gbuf[ring], preferred_element_type=F32)
                up = jnp.dot(rows, ubuf[ring], preferred_element_type=F32)
                hbuf[side, 0:size, columns(f)] = (jax.nn.silu(gate) * up).astype(BF16)

            sized(total, run)

            @pl.when(step + W_SLOTS < steps)
            def _more():
                start_w(step + W_SLOTS)

            return _

        lax.fori_loop(0, f_tiles, gate_up, 0)

        def down(f, _):
            step = e * d_tiles + f
            ring = lax.rem(step, DN_SLOTS)
            d_copy(step).wait()

            def run(size):
                xbuf[slot, 0:size, columns(f)] = jnp.dot(hbuf[side, 0:size, :], dbuf[ring],
                                                         preferred_element_type=F32).astype(BF16)

            sized(total, run)

            @pl.when(step + DN_SLOTS < d_steps)
            def _more():
                d_copy(step + DN_SLOTS).start()

            return _

        if early > 0:
            @pl.when(e < early)
            def _down():
                lax.fori_loop(0, d_tiles, down, 0)
                each_chunk(e, lambda p, j, i: o_copy(e, p, j, slot, i).start())

        if early < experts:
            @pl.when(e >= early)
            def _keep():
                start_h(e, side)

        return _

    lax.fori_loop(0, experts, expert, 0)
    for e in range(max(0, experts - 2), experts):
        if e < early:
            wait_rows(e, e % 3, lambda *a: o_copy(*a))
    for e in range(max(early, experts - 2), experts):
        wait_h(e % 2)


def combine_kernel(tok, win, early, o_hbm, h_hbm, c_hbm, wd_hbm, out_ref,
                   hbuf, cbuf, wbuf, obuf, ysend, zbuf, pbuf, fbuf, nbuf,
                   h_sem, c_sem, w_sem, o_sem, y_send, y_recv, far_send, far_recv, near_send, near_recv):
    me, chip, core, right, left, far = ring_places()
    experts, chips, pair_rows, _ = o_hbm.shape
    late = experts - early
    blocks = out_ref.shape[1] // WIDE
    halves = WIDE // COL
    steps = blocks * late
    partner = chip * 2 + 1 - core
    right_dev, left_dev = right * 2 + core, left * 2 + core
    dests = (far, right, left, chip)
    cut = tok // 2

    def wide(b):
        return pl.ds(pl.multiple_of(b * WIDE, WIDE), WIDE)

    def w_copy(step):
        b, e, slot = step // late, early + lax.rem(step, late), lax.rem(step, D_SLOTS)
        return pltpu.make_async_copy(wd_hbm.at[e, :, wide(b)], wbuf.at[slot], w_sem.at[slot])

    def h_copy(e):
        return pltpu.make_async_copy(h_hbm.at[e], hbuf.at[e], h_sem.at[e])

    def o_copies(b):
        slot = lax.rem(b, 2)
        return [pltpu.make_async_copy(o_hbm.at[0:early, p, pl.ds(side * (pair_rows - win), win), wide(b)],
                                      obuf.at[slot, 2 * p + side, 0:early], o_sem.at[slot, 2 * p + side])
                for p in range(chips) for side in range(2)]

    c_copy = pltpu.make_async_copy(c_hbm, cbuf, c_sem)
    if early > 0:
        for copy in o_copies(jnp.int32(0)):
            copy.start()
    for e in range(late):
        h_copy(e).start()
        if e < D_SLOTS:
            w_copy(jnp.int32(e)).start()
    c_copy.start()
    if late > 0:
        for s in range(late, min(D_SLOTS, steps)):
            w_copy(jnp.int32(s)).start()

    barrier = pltpu.get_barrier_semaphore()
    for dev in (partner, right_dev, left_dev):
        pl.semaphore_signal(barrier, inc=1, device_id={'ep': dev}, device_id_type=MESH)
    pl.semaphore_wait(barrier, 3)

    def y_copy(b, d):
        return remote(ysend.at[lax.rem(b, 2), d], pbuf.at[b, d], y_send.at[lax.rem(b, 2), d], y_recv.at[b, d], partner)

    def far_copy(b, i, side):
        src = zbuf.at[lax.rem(b, Z_SLOTS), 0, i, pl.ds(side * cut, cut), :]
        slot = 2 * i + side
        return remote(src, fbuf.at[b, slot], far_send.at[b, slot], far_recv.at[b, slot], (right_dev, left_dev)[side])

    def near_copy(b, i, side):
        src = zbuf.at[lax.rem(b, Z_SLOTS), 1 + side, i]
        slot = 2 * i + side
        return remote(src, nbuf.at[b, slot], near_send.at[b, slot], near_recv.at[b, slot], (right_dev, left_dev)[side])

    def gated(b, s):
        rows = obuf[lax.rem(b, 2), s].reshape(experts * win, WIDE)
        three = jnp.dot(cbuf[s], rows, preferred_element_type=F32)
        return three[0:tok] + three[tok:2 * tok] + three[2 * tok:3 * tok]

    def project(b):
        if early > 0:
            @pl.when(b + 1 < blocks)
            def _ahead():
                for copy in o_copies(b + 1):
                    copy.start()

        def one(e, _):
            step = b * late + e

            @pl.when(b == 0)
            def _first():
                h_copy(e).wait()

            w_copy(step).wait()
            o = jnp.dot(hbuf[e], wbuf[lax.rem(step, D_SLOTS)], preferred_element_type=F32).astype(BF16)
            for p in range(chips):
                obuf[lax.rem(b, 2), 2 * p, early + e] = o[p * pair_rows:p * pair_rows + win]
                obuf[lax.rem(b, 2), 2 * p + 1, early + e] = o[(p + 1) * pair_rows - win:(p + 1) * pair_rows]

            @pl.when(step + D_SLOTS < steps)
            def _more():
                w_copy(step + D_SLOTS).start()

            return _

        if late > 0:
            lax.fori_loop(0, late, one, 0)
        if early > 0:
            for copy in o_copies(b):
                copy.wait()

    def pass_on(b):
        for i in range(halves):
            for side in range(2):
                far_copy(b, i, side).wait_recv()
                part = pl.ds(side * cut, cut)
                zbuf[lax.rem(b, Z_SLOTS), 1 + side, i, part, :] += fbuf[b, 2 * i + side]
                near_copy(b, i, side).start()

    def sums(b):
        @pl.when(b >= 2)
        def _reuse():
            for d in range(4):
                y_copy(b - 2, d).wait_send()

        def give(d):
            y = gated(b, 2 * dests[d] + 1 - core)
            for i in range(halves):
                ysend[lax.rem(b, 2), d, i] = y[:, i * COL:(i + 1) * COL]
            y_copy(b, d).start()

        def take(d):
            y_copy(b, d).wait_recv()
            zbuf[lax.rem(b, Z_SLOTS), d] += pbuf[b, d]
            if d == 0:
                for i in range(halves):
                    far_copy(b, i, 0).start()
                    far_copy(b, i, 1).start()

        give(0)
        for d in range(4):
            y = gated(b, 2 * dests[d] + core)
            for i in range(halves):
                zbuf[lax.rem(b, Z_SLOTS), d, i] = y[:, i * COL:(i + 1) * COL]
            if d < 3:
                give(d + 1)
            if d > 0:
                take(d - 1)
        take(3)

    def finish(b):
        for i in range(halves):
            near_copy(b, i, 0).wait_recv()
            near_copy(b, i, 1).wait_recv()
            total = zbuf[lax.rem(b, Z_SLOTS), 3, i] + nbuf[b, 2 * i] + nbuf[b, 2 * i + 1]
            out_ref[:, pl.ds(pl.multiple_of(b * WIDE + i * COL, COL), COL)] = total.astype(out_ref.dtype)
        for i in range(halves):
            for side in range(2):
                far_copy(b, i, side).wait_send()
                near_copy(b, i, side).wait_send()

    def body(b, _):
        @pl.when(b < blocks)
        def _project():
            project(b)

        @pl.when(b == 0)
        def _gates():
            c_copy.wait()

        @pl.when((b >= 1) & (b <= blocks))
        def _pass_on():
            pass_on(b - 1)

        @pl.when(b >= 2)
        def _finish():
            finish(b - 2)

        @pl.when(b < blocks)
        def _sums():
            sums(b)

        return _

    lax.fori_loop(0, blocks + 2, body, 0)
    for back in (2, 1):
        for d in range(4):
            y_copy(jnp.int32(blocks - back), d).wait_send()


def solution(mesh):
    ep_size = mesh.shape['ep']
    chips = ep_size // 2

    def device_body(hidden, route_idx, gate_weights, w_gate, w_up, w_down):
        tok, top_k = route_idx.shape
        d_model = hidden.shape[1]
        experts, _, d_ff = w_gate.shape
        num_experts = experts * ep_size
        cap = min(tok, 4 * top_k * tok // num_experts)
        pair_rows = 2 * cap
        win = (cap + CHUNK - 1) // CHUNK * CHUNK
        tiles = d_model // COL
        blocks, halves = d_model // WIDE, WIDE // COL
        rows = chips * pair_rows
        any_space = pl.BlockSpec(memory_space=pl.ANY)
        vmem = pl.BlockSpec(memory_space=pltpu.VMEM)
        dma = pltpu.SemaphoreType.DMA

        meta = jnp.concatenate([route_idx.T.astype(F32) + 1.0, gate_weights.T], axis=1)
        meta = jnp.pad(meta, ((0, 8 - top_k), (0, 0)))

        xs, gates, counts = pl.pallas_call(
            functools.partial(dispatch_kernel, tok, cap, win),
            out_shape=(jax.ShapeDtypeStruct((experts, chips, pair_rows, d_model), BF16),
                       jax.ShapeDtypeStruct((ep_size, 3 * tok, experts * win), BF16),
                       jax.ShapeDtypeStruct((experts, 128), jnp.int32)),
            in_specs=[any_space, vmem],
            out_specs=(any_space, any_space, vmem),
            scratch_shapes=[
                pltpu.VMEM((ep_size, tok, d_model), BF16),
                pltpu.VMEM((ep_size, 8, 2 * tok), F32),
                pltpu.VMEM((chips, experts * pair_rows, 2 * tok), BF16),
                pltpu.VMEM((chips, experts, pair_rows, d_model), BF16),
                pltpu.VMEM((ep_size, 3 * tok, experts * win), BF16),
                pltpu.VMEM((2 * tok, 2 * tok), BF16),
                dma((2,)), dma((7,)), dma((7,)),
                dma((tiles + tiles // 2,)), dma((tiles + tiles // 2,)), dma((tiles + tiles // 2,)), dma((tiles + tiles // 2,)),
                dma((4 * tiles,)), dma((4 * tiles,)), dma((chips, tiles)), dma,
            ],
            compiler_params=pltpu.CompilerParams(collective_id=0, has_side_effects=True, vmem_limit_bytes=VMEM_LIMIT),
            name='dispatch',
        )(hidden, meta)

        early = min(EARLY, experts)
        late = experts - early
        held = max(late, 1)
        outs, act = pl.pallas_call(
            functools.partial(ffn_kernel, cap, early),
            out_shape=(jax.ShapeDtypeStruct(xs.shape, BF16),
                       jax.ShapeDtypeStruct((held, chips, pair_rows, d_ff), BF16)),
            in_specs=[pl.BlockSpec(memory_space=pltpu.SMEM)] + [any_space] * 4,
            out_specs=(any_space, any_space),
            scratch_shapes=[
                pltpu.VMEM((3, rows, d_model), BF16),
                pltpu.VMEM((W_SLOTS, d_model, FCOL), BF16),
                pltpu.VMEM((W_SLOTS, d_model, FCOL), BF16),
                pltpu.VMEM((DN_SLOTS, d_ff, FCOL), BF16),
                pltpu.VMEM((2, rows, d_ff), BF16),
                pltpu.VMEM((CHUNK, d_ff), BF16),
                dma((3, rows // CHUNK)), dma((W_SLOTS, 2)), dma((DN_SLOTS,)), dma((2, chips, pair_rows // CHUNK)),
            ],
            input_output_aliases={1: 0},
            compiler_params=pltpu.CompilerParams(vmem_limit_bytes=VMEM_LIMIT),
            name='experts',
        )(counts, xs, w_gate, w_up, w_down)

        return pl.pallas_call(
            functools.partial(combine_kernel, tok, win, early),
            out_shape=jax.ShapeDtypeStruct((tok, d_model), BF16),
            in_specs=[any_space] * 4,
            out_specs=vmem,
            scratch_shapes=[
                pltpu.VMEM((held, rows, d_ff), BF16),
                pltpu.VMEM((ep_size, 3 * tok, experts * win), BF16),
                pltpu.VMEM((D_SLOTS, d_ff, WIDE), BF16),
                pltpu.VMEM((2, ep_size, experts, win, WIDE), BF16),
                pltpu.VMEM((2, chips, halves, tok, COL), F32),
                pltpu.VMEM((Z_SLOTS, chips, halves, tok, COL), F32),
                pltpu.VMEM((blocks, chips, halves, tok, COL), F32),
                pltpu.VMEM((blocks, 2 * halves, tok // 2, COL), F32),
                pltpu.VMEM((blocks, 2 * halves, tok, COL), F32),
                dma((held,)), dma, dma((D_SLOTS,)), dma((2, ep_size)),
                dma((2, chips)), dma((blocks, chips)),
                dma((blocks, 2 * halves)), dma((blocks, 2 * halves)), dma((blocks, 2 * halves)), dma((blocks, 2 * halves)),
            ],
            compiler_params=pltpu.CompilerParams(collective_id=1, has_side_effects=True, vmem_limit_bytes=VMEM_LIMIT),
            name='down_combine',
        )(outs, act.reshape(held, rows, d_ff), gates, w_down)

    row_spec = P(('dp', 'ep'), None)
    expert_spec = P('ep', None, None)
    return jax.shard_map(device_body, mesh=mesh, in_specs=(row_spec, row_spec, row_spec, expert_spec, expert_spec, expert_spec), out_specs=row_spec, check_vma=False)
```

```python
import functools

import jax
import jax.numpy as jnp
from jax import lax
from jax.experimental import pallas as pl
from jax.experimental.pallas import tpu as pltpu
from jax.sharding import PartitionSpec as P

MESH = pl.DeviceIdType.MESH
BF16 = jnp.bfloat16
F32 = jnp.float32
COL = 256
WIDE = 512
FCOL = 512
CHUNK = 16
W_SLOTS = 4
DN_SLOTS = 6
D_SLOTS = 6
EARLY = 3
Z_SLOTS = 3
VMEM_LIMIT = 63_000_000


def ring_places():
    me = lax.axis_index('ep')
    chip = me // 2
    core = lax.rem(me, 2)
    right = lax.rem(chip + 1, 4)
    far = lax.rem(chip + 2, 4)
    left = lax.rem(chip + 3, 4)
    return me, chip, core, right, left, far


def remote(src, dst, send_sem, recv_sem, device):
    return pltpu.make_async_remote_copy(src_ref=src, dst_ref=dst, send_sem=send_sem, recv_sem=recv_sem,
                                        device_id={'ep': device}, device_id_type=MESH)


def dispatch_kernel(tok, cap, win, x_hbm, meta_ref, xs_hbm, c_hbm, cnt_ref,
                    xbuf, mbuf, gbuf, stage, cstage, upper,
                    local_sem, meta_send, meta_recv, plus_send, plus_recv, minus_send, minus_recv,
                    pair_send, pair_recv, xs_sem, c_sem):
    me, chip, core, right, left, far = ring_places()
    n_dev = xbuf.shape[0]
    local_experts, _, pair_rows, d_model = xs_hbm.shape
    tiles = d_model // COL
    half = tiles // 2
    partner = chip * 2 + 1 - core
    right_dev, left_dev = right * 2 + core, left * 2 + core

    own_copy = pltpu.make_async_copy(x_hbm, xbuf.at[me], local_sem.at[0])
    own_copy.start()
    meta_copy = pltpu.make_async_copy(meta_ref, mbuf.at[me], local_sem.at[1])
    meta_copy.start()

    far_same = far * 2 + core
    barrier = pltpu.get_barrier_semaphore()
    for dev in (partner, right_dev, left_dev, far_same):
        pl.semaphore_signal(barrier, inc=1, device_id={'ep': dev}, device_id_type=MESH)
    pl.semaphore_wait(barrier, 4)

    def meta_send_to(slot, source, device):
        return remote(mbuf.at[source], mbuf.at[source], meta_send.at[slot], meta_recv.at[slot], device)

    meta_copy.wait()
    for slot, dev in enumerate((right_dev, left_dev, far_same, partner)):
        meta_send_to(slot, me, dev).start()
    own_copy.wait()

    def cols(j):
        return pl.ds(pl.multiple_of(j * COL, COL), COL)

    def block(dev, j):
        return xbuf.at[dev, :, cols(j)]

    def plus(j, slot, dev):
        return remote(block(dev, j), block(dev, j), plus_send.at[slot], plus_recv.at[slot], right_dev)

    def minus(j, slot, dev):
        return remote(block(dev, j), block(dev, j), minus_send.at[slot], minus_recv.at[slot], left_dev)

    def pair(j, group, dev):
        slot = group * tiles + j
        return remote(block(dev, j), block(dev, j), pair_send.at[slot], pair_recv.at[slot], partner)

    def send_own(j, _):
        plus(j, j, me).start()
        other = lax.rem(j + half, tiles)
        minus(other, other, me).start()
        pair(j, 0, me).start()
        return _

    lax.fori_loop(0, tiles, send_own, 0)

    row_i = lax.broadcasted_iota(jnp.int32, upper.shape, 0)
    col_i = lax.broadcasted_iota(jnp.int32, upper.shape, 1)
    same = (row_i < tok) == (col_i < tok)
    upper[...] = jnp.where((row_i < col_i) & same, 1.0, 0.0).astype(BF16)

    for slot, dev in enumerate((left_dev, right_dev, far_same)):
        meta_send_to(slot, dev, partner).wait_recv()
        meta_send_to(4 + slot, dev, partner).start()
    for slot, q in ((3, chip), (4, left), (5, right), (6, far)):
        meta_send_to(slot, 2 * q + 1 - core, partner).wait_recv()

    def plan(q, counts):
        one, two = mbuf[2 * q], mbuf[2 * q + 1]
        both = one.shape[1]
        low = lax.broadcasted_iota(jnp.int32, one.shape, 1) < tok
        ids = jnp.where(low, one, pltpu.roll(two, tok, 1))
        weights = jnp.where(low, pltpu.roll(one, tok, 1), two)
        target = (lax.broadcasted_iota(jnp.int32, (local_experts, both), 0) + (me * local_experts + 1)).astype(F32)
        chosen = jnp.zeros((local_experts, both), F32)
        gates = jnp.zeros((local_experts, both), F32)
        for k in range(ids.shape[0]):
            hit = jnp.broadcast_to(ids[k:k + 1, :], (local_experts, both)) == target
            chosen = jnp.where(hit, 1.0, chosen)
            gates = jnp.where(hit, jnp.broadcast_to(weights[k:k + 1, :], (local_experts, both)), gates)
        rank = jnp.dot(chosen.astype(BF16), upper[...], preferred_element_type=F32)
        lane = lax.broadcasted_iota(jnp.int32, (local_experts, both), 1)
        first = lane < tok
        place = jnp.where(first, (cap - 1) - rank, cap + rank)
        place = jnp.where(chosen > 0, place, -4096.0)
        count0 = jnp.sum(jnp.where(first, chosen, 0.0), axis=1, keepdims=True)
        count1 = jnp.sum(jnp.where(first, 0.0, chosen), axis=1, keepdims=True)
        out_lane = lax.broadcasted_iota(jnp.int32, counts.shape, 1)
        counts = jnp.where(out_lane == 2 * q, count0, counts)
        counts = jnp.where(out_lane == 2 * q + 1, count1, counts)

        slot_i = lax.broadcasted_iota(jnp.int32, (pair_rows, both), 0).astype(F32)
        for e in range(local_experts):
            gbuf[q, e * pair_rows:(e + 1) * pair_rows, :] = jnp.where(slot_i == place[e:e + 1, :], 1.0, 0.0).astype(BF16)

        turned = jnp.concatenate([place, gates, jnp.zeros((128 - 2 * local_experts, both), F32)], axis=0).T
        for side in range(2):
            part = turned[side * tok:(side + 1) * tok, :]
            offset = 0 if side == 0 else pair_rows - win
            for lt in range(local_experts * win // 128):
                lanes = (lax.broadcasted_iota(jnp.int32, (tok, 128), 1) + lt * 128).astype(F32)
                acc = jnp.zeros((tok, 128), F32)
                for e in range(local_experts):
                    if e * win < (lt + 1) * 128 and (e + 1) * win > lt * 128:
                        acc = jnp.where(lanes == part[:, e:e + 1] + float(e * win - offset),
                                        part[:, local_experts + e:local_experts + e + 1], acc)
                hi = acc.astype(BF16)
                rest = acc - hi.astype(F32)
                mid = rest.astype(BF16)
                tail = (rest - mid.astype(F32)).astype(BF16)
                where = slice(lt * 128, (lt + 1) * 128)
                cstage[2 * q + side, 0:tok, where] = hi
                cstage[2 * q + side, tok:2 * tok, where] = mid
                cstage[2 * q + side, 2 * tok:3 * tok, where] = tail
        return counts

    counts = lax.fori_loop(0, n_dev // 2, plan, jnp.zeros(cnt_ref.shape, F32))
    cnt_ref[...] = counts.astype(jnp.int32)
    c_copy = pltpu.make_async_copy(cstage, c_hbm, c_sem)
    c_copy.start()

    def xs_copy(q, j):
        return pltpu.make_async_copy(stage.at[q, :, :, cols(j)], xs_hbm.at[:, q, :, cols(j)], xs_sem.at[q, j])

    def pick(q, j):
        rows = xbuf[pl.ds(2 * q, 2), :, cols(j)].reshape(2 * tok, COL)
        hold = local_experts // 2
        for part in range(2):
            sel = gbuf[q, part * hold * pair_rows:(part + 1) * hold * pair_rows, :]
            got = jnp.dot(sel, rows, preferred_element_type=F32).astype(BF16)
            stage[q, part * hold:(part + 1) * hold, :, cols(j)] = got.reshape(hold, pair_rows, COL)
        xs_copy(q, j).start()

    def pick_own(j, _):
        pair(j, 0, partner).wait_recv()
        pick(chip, j)
        return _

    lax.fori_loop(0, tiles, pick_own, 0)

    def near_a(i, _):
        plus(i, i, left_dev).wait_recv()
        plus(i, tiles + i, left_dev).start()
        pair(i, 1, left_dev).start()
        j = half + i
        minus(j, j, right_dev).wait_recv()
        minus(j, tiles + i, right_dev).start()
        pair(j, 2, right_dev).start()
        return _

    lax.fori_loop(0, half, near_a, 0)

    left_other, right_other = left * 2 + 1 - core, right * 2 + 1 - core

    def near_b(i, _):
        j = half + i
        plus(j, j, left_dev).wait_recv()
        pair(j, 1, left_dev).start()
        minus(i, i, right_dev).wait_recv()
        pair(i, 2, right_dev).start()
        pair(i, 1, left_other).wait_recv()
        pick(left, i)
        pair(j, 2, right_other).wait_recv()
        pick(right, j)

        @pl.when(i > 0)
        def _late():
            pair(j - 1, 1, left_other).wait_recv()
            pick(left, j - 1)
            pair(i - 1, 2, right_other).wait_recv()
            pick(right, i - 1)

        return _

    lax.fori_loop(0, half, near_b, 0)
    pair(tiles - 1, 1, left_other).wait_recv()
    pick(left, tiles - 1)
    pair(half - 1, 2, right_other).wait_recv()
    pick(right, half - 1)

    far_dev, far_other = far * 2 + core, far * 2 + 1 - core

    def far_c(i, _):
        @pl.when(i < half)
        def _arrive():
            plus(i, tiles + i, far_dev).wait_recv()
            pair(i, 3, far_dev).start()
            minus(half + i, tiles + i, far_dev).wait_recv()
            pair(half + i, 3, far_dev).start()

        @pl.when(i > 0)
        def _late():
            pair(i - 1, 3, far_other).wait_recv()
            pick(far, i - 1)
            pair(half + i - 1, 3, far_other).wait_recv()
            pick(far, half + i - 1)

        return _

    lax.fori_loop(0, half + 1, far_c, 0)

    for slot in range(7):
        meta_send_to(slot, me, partner).wait_send()

    def drain_ring(s, _):
        plus(0, s, me).wait_send()
        minus(0, s, me).wait_send()
        return _

    lax.fori_loop(0, tiles + half, drain_ring, 0)

    def drain_pair(s, _):
        for group in range(4):
            pair(s, group, me).wait_send()
        for q in range(n_dev // 2):
            xs_copy(q, s).wait()
        return _

    lax.fori_loop(0, tiles, drain_pair, 0)
    c_copy.wait()


def ffn_kernel(cap, early, cnt_ref, xs_hbm, wg_hbm, wu_hbm, wd_hbm, out_hbm, h_hbm,
               xbuf, gbuf, ubuf, dbuf, hbuf, zbuf, x_sem, w_sem, d_sem, h_sem):
    experts, chips, pair_rows, d_model = xs_hbm.shape
    d_ff = hbuf.shape[2]
    f_tiles, d_tiles = d_ff // FCOL, d_model // FCOL
    steps = experts * f_tiles
    d_steps = early * d_tiles
    per_chip = pair_rows // CHUNK
    all_rows = chips * pair_rows
    zbuf[...] = jnp.zeros_like(zbuf)

    def chunk_range(e, p):
        lo = (cap - cnt_ref[e, 2 * p]) // CHUNK
        hi = (cap + cnt_ref[e, 2 * p + 1] + (CHUNK - 1)) // CHUNK
        return lo, hi

    def chunk(i):
        return pl.ds(pl.multiple_of(i * CHUNK, CHUNK), CHUNK)

    def chunk_total(e):
        total = jnp.int32(0)
        for p in range(chips):
            lo, hi = chunk_range(e, p)
            total = total + (hi - lo)
        return total

    def each_chunk(e, act):
        base = jnp.int32(0)
        for p in range(chips):
            lo, hi = chunk_range(e, p)

            def one(j, _, p=p, lo=lo, base=base):
                act(p, j, base + j - lo)
                return _

            lax.fori_loop(lo, hi, one, 0)
            base = base + (hi - lo)

    def x_copy(e, p, j, slot, i):
        return pltpu.make_async_copy(xs_hbm.at[e, p, chunk(j), :], xbuf.at[slot, chunk(i), :], x_sem.at[slot, i])

    def o_copy(e, p, j, slot, i):
        return pltpu.make_async_copy(xbuf.at[slot, chunk(i), :], out_hbm.at[e, p, chunk(j), :], x_sem.at[slot, i])

    def wait_rows(e, slot, copy):
        def one(i, _):
            copy(0, 0, 0, slot, i).wait()
            return _

        lax.fori_loop(0, chunk_total(e), one, 0)

    def start_x(e):
        slot = lax.rem(e, 3)
        each_chunk(e, lambda p, j, i: x_copy(e, p, j, slot, i).start())

    def w_copies(step):
        e, f, slot = step // f_tiles, lax.rem(step, f_tiles), lax.rem(step, W_SLOTS)
        where = pl.ds(pl.multiple_of(f * FCOL, FCOL), FCOL)
        return (pltpu.make_async_copy(wg_hbm.at[e, :, where], gbuf.at[slot], w_sem.at[slot, 0]),
                pltpu.make_async_copy(wu_hbm.at[e, :, where], ubuf.at[slot], w_sem.at[slot, 1]))

    def start_w(step):
        for copy in w_copies(step):
            copy.start()

    def d_copy(step):
        e, f, slot = step // d_tiles, lax.rem(step, d_tiles), lax.rem(step, DN_SLOTS)
        where = pl.ds(pl.multiple_of(f * FCOL, FCOL), FCOL)
        return pltpu.make_async_copy(wd_hbm.at[e, :, where], dbuf.at[slot], d_sem.at[slot])

    def start_h(e, slot):
        base = jnp.int32(0)
        for p in range(chips):
            lo, hi = chunk_range(e, p)

            def one(j, _, p=p, lo=lo, hi=hi, base=base):
                live = (j >= lo) & (j < hi)

                @pl.when(live)
                def _live():
                    pltpu.make_async_copy(hbuf.at[slot, chunk(base + j - lo), :], h_hbm.at[e - early, p, chunk(j), :],
                                          h_sem.at[slot, p, j]).start()

                @pl.when(jnp.logical_not(live))
                def _dead():
                    pltpu.make_async_copy(zbuf, h_hbm.at[e - early, p, chunk(j), :], h_sem.at[slot, p, j]).start()

                return _

            lax.fori_loop(0, per_chip, one, 0)
            base = base + (hi - lo)

    def wait_h(slot):
        for p in range(chips):

            def one(j, _, p=p):
                pltpu.make_async_copy(zbuf, h_hbm.at[0, p, chunk(j), :], h_sem.at[slot, p, j]).wait()
                return _

            lax.fori_loop(0, per_chip, one, 0)

    start_x(jnp.int32(0))
    for s in range(min(W_SLOTS, steps)):
        start_w(jnp.int32(s))
        if s < min(DN_SLOTS, d_steps) and s < f_tiles:
            d_copy(jnp.int32(s)).start()
    for s in range(min(W_SLOTS, f_tiles), min(DN_SLOTS, d_steps)):
        d_copy(jnp.int32(s)).start()

    sizes = sorted({min(all_rows, m) for m in (128, 160, 192, 224, 256, 384, all_rows)})

    def sized(total, run):
        below = 0
        for size in sizes:
            @pl.when((total > below) & (total <= size // CHUNK))
            def _run(size=size):
                run(size)

            below = size // CHUNK

    def columns(f):
        return pl.ds(pl.multiple_of(f * FCOL, FCOL), FCOL)

    def expert(e, _):
        slot, side = lax.rem(e, 3), lax.rem(e, 2)
        total = chunk_total(e)

        @pl.when((e >= 2) & (e - 2 < early))
        def _sent():
            wait_rows(e - 2, lax.rem(e - 2, 3), lambda *a: o_copy(*a))

        @pl.when(e + 1 < experts)
        def _next():
            start_x(e + 1)

        wait_rows(e, slot, lambda *a: x_copy(*a))

        if early < experts:
            @pl.when(e - 2 >= early)
            def _reuse():
                wait_h(side)

        def gate_up(f, _):
            step = e * f_tiles + f
            ring = lax.rem(step, W_SLOTS)
            for copy in w_copies(step):
                copy.wait()

            def run(size):
                rows = xbuf[slot, 0:size, :]
                gate = jnp.dot(rows, gbuf[ring], preferred_element_type=F32)
                up = jnp.dot(rows, ubuf[ring], preferred_element_type=F32)
                hbuf[side, 0:size, columns(f)] = (jax.nn.silu(gate) * up).astype(BF16)

            sized(total, run)

            @pl.when(step + W_SLOTS < steps)
            def _more():
                start_w(step + W_SLOTS)

            return _

        lax.fori_loop(0, f_tiles, gate_up, 0)

        def down(f, _):
            step = e * d_tiles + f
            ring = lax.rem(step, DN_SLOTS)
            d_copy(step).wait()

            def run(size):
                xbuf[slot, 0:size, columns(f)] = jnp.dot(hbuf[side, 0:size, :], dbuf[ring],
                                                         preferred_element_type=F32).astype(BF16)

            sized(total, run)

            @pl.when(step + DN_SLOTS < d_steps)
            def _more():
                d_copy(step + DN_SLOTS).start()

            return _

        if early > 0:
            @pl.when(e < early)
            def _down():
                lax.fori_loop(0, d_tiles, down, 0)
                each_chunk(e, lambda p, j, i: o_copy(e, p, j, slot, i).start())

        if early < experts:
            @pl.when(e >= early)
            def _keep():
                start_h(e, side)

        return _

    lax.fori_loop(0, experts, expert, 0)
    for e in range(max(0, experts - 2), experts):
        if e < early:
            wait_rows(e, e % 3, lambda *a: o_copy(*a))
    for e in range(max(early, experts - 2), experts):
        wait_h(e % 2)


def combine_kernel(tok, win, early, o_hbm, h_hbm, c_hbm, wd_hbm, out_ref,
                   hbuf, cbuf, wbuf, obuf, ysend, zbuf, pbuf, fbuf, nbuf,
                   h_sem, c_sem, w_sem, o_sem, y_send, y_recv, far_send, far_recv, near_send, near_recv):
    me, chip, core, right, left, far = ring_places()
    experts, chips, pair_rows, _ = o_hbm.shape
    late = experts - early
    blocks = out_ref.shape[1] // WIDE
    halves = WIDE // COL
    steps = blocks * late
    partner = chip * 2 + 1 - core
    right_dev, left_dev = right * 2 + core, left * 2 + core
    dests = (far, right, left, chip)
    cut = tok // 2

    def wide(b):
        return pl.ds(pl.multiple_of(b * WIDE, WIDE), WIDE)

    def w_copy(step):
        b, e, slot = step // late, early + lax.rem(step, late), lax.rem(step, D_SLOTS)
        return pltpu.make_async_copy(wd_hbm.at[e, :, wide(b)], wbuf.at[slot], w_sem.at[slot])

    def h_copy(e):
        return pltpu.make_async_copy(h_hbm.at[e], hbuf.at[e], h_sem.at[e])

    def o_copies(b):
        slot = lax.rem(b, 2)
        return [pltpu.make_async_copy(o_hbm.at[0:early, p, pl.ds(side * (pair_rows - win), win), wide(b)],
                                      obuf.at[slot, 2 * p + side, 0:early], o_sem.at[slot, 2 * p + side])
                for p in range(chips) for side in range(2)]

    c_copy = pltpu.make_async_copy(c_hbm, cbuf, c_sem)
    if early > 0:
        for copy in o_copies(jnp.int32(0)):
            copy.start()
    for e in range(late):
        h_copy(e).start()
        if e < D_SLOTS:
            w_copy(jnp.int32(e)).start()
    c_copy.start()
    if late > 0:
        for s in range(late, min(D_SLOTS, steps)):
            w_copy(jnp.int32(s)).start()

    barrier = pltpu.get_barrier_semaphore()
    for dev in (partner, right_dev, left_dev):
        pl.semaphore_signal(barrier, inc=1, device_id={'ep': dev}, device_id_type=MESH)
    pl.semaphore_wait(barrier, 3)

    def y_copy(b, d):
        return remote(ysend.at[lax.rem(b, 2), d], pbuf.at[b, d], y_send.at[lax.rem(b, 2), d], y_recv.at[b, d], partner)

    def far_copy(b, i, side):
        src = zbuf.at[lax.rem(b, Z_SLOTS), 0, i, pl.ds(side * cut, cut), :]
        slot = 2 * i + side
        return remote(src, fbuf.at[b, slot], far_send.at[b, slot], far_recv.at[b, slot], (right_dev, left_dev)[side])

    def near_copy(b, i, side):
        src = zbuf.at[lax.rem(b, Z_SLOTS), 1 + side, i]
        slot = 2 * i + side
        return remote(src, nbuf.at[b, slot], near_send.at[b, slot], near_recv.at[b, slot], (right_dev, left_dev)[side])

    def gated(b, s):
        rows = obuf[lax.rem(b, 2), s].reshape(experts * win, WIDE)
        three = jnp.dot(cbuf[s], rows, preferred_element_type=F32)
        return three[0:tok] + three[tok:2 * tok] + three[2 * tok:3 * tok]

    def project(b):
        if early > 0:
            @pl.when(b + 1 < blocks)
            def _ahead():
                for copy in o_copies(b + 1):
                    copy.start()

        def one(e, _):
            step = b * late + e

            @pl.when(b == 0)
            def _first():
                h_copy(e).wait()

            w_copy(step).wait()
            o = jnp.dot(hbuf[e], wbuf[lax.rem(step, D_SLOTS)], preferred_element_type=F32).astype(BF16)
            for p in range(chips):
                obuf[lax.rem(b, 2), 2 * p, early + e] = o[p * pair_rows:p * pair_rows + win]
                obuf[lax.rem(b, 2), 2 * p + 1, early + e] = o[(p + 1) * pair_rows - win:(p + 1) * pair_rows]

            @pl.when(step + D_SLOTS < steps)
            def _more():
                w_copy(step + D_SLOTS).start()

            return _

        if late > 0:
            lax.fori_loop(0, late, one, 0, unroll=True)
        if early > 0:
            for copy in o_copies(b):
                copy.wait()

    def pass_on(b):
        for i in range(halves):
            for side in range(2):
                far_copy(b, i, side).wait_recv()
                part = pl.ds(side * cut, cut)
                zbuf[lax.rem(b, Z_SLOTS), 1 + side, i, part, :] += fbuf[b, 2 * i + side]
                near_copy(b, i, side).start()

    def sums(b):
        @pl.when(b >= 2)
        def _reuse():
            for d in range(4):
                y_copy(b - 2, d).wait_send()

        def give(d):
            y = gated(b, 2 * dests[d] + 1 - core)
            for i in range(halves):
                ysend[lax.rem(b, 2), d, i] = y[:, i * COL:(i + 1) * COL]
            y_copy(b, d).start()

        def take(d):
            y_copy(b, d).wait_recv()
            zbuf[lax.rem(b, Z_SLOTS), d] += pbuf[b, d]
            if d == 0:
                for i in range(halves):
                    far_copy(b, i, 0).start()
                    far_copy(b, i, 1).start()

        give(0)
        for d in range(4):
            y = gated(b, 2 * dests[d] + core)
            for i in range(halves):
                zbuf[lax.rem(b, Z_SLOTS), d, i] = y[:, i * COL:(i + 1) * COL]
            if d < 3:
                give(d + 1)
            if d > 0:
                take(d - 1)
        take(3)

    def finish(b):
        for i in range(halves):
            near_copy(b, i, 0).wait_recv()
            near_copy(b, i, 1).wait_recv()
            total = zbuf[lax.rem(b, Z_SLOTS), 3, i] + nbuf[b, 2 * i] + nbuf[b, 2 * i + 1]
            out_ref[:, pl.ds(pl.multiple_of(b * WIDE + i * COL, COL), COL)] = total.astype(out_ref.dtype)
        for i in range(halves):
            for side in range(2):
                far_copy(b, i, side).wait_send()
                near_copy(b, i, side).wait_send()

    def body(b, _):
        @pl.when(b < blocks)
        def _project():
            project(b)

        @pl.when(b == 0)
        def _gates():
            c_copy.wait()

        @pl.when((b >= 1) & (b <= blocks))
        def _pass_on():
            pass_on(b - 1)

        @pl.when(b >= 2)
        def _finish():
            finish(b - 2)

        @pl.when(b < blocks)
        def _sums():
            sums(b)

        return _

    lax.fori_loop(0, blocks + 2, body, 0)
    for back in (2, 1):
        for d in range(4):
            y_copy(jnp.int32(blocks - back), d).wait_send()


def solution(mesh):
    ep_size = mesh.shape['ep']
    chips = ep_size // 2

    def device_body(hidden, route_idx, gate_weights, w_gate, w_up, w_down):
        tok, top_k = route_idx.shape
        d_model = hidden.shape[1]
        experts, _, d_ff = w_gate.shape
        num_experts = experts * ep_size
        cap = min(tok, 4 * top_k * tok // num_experts)
        pair_rows = 2 * cap
        win = (cap + CHUNK - 1) // CHUNK * CHUNK
        tiles = d_model // COL
        blocks, halves = d_model // WIDE, WIDE // COL
        rows = chips * pair_rows
        any_space = pl.BlockSpec(memory_space=pl.ANY)
        vmem = pl.BlockSpec(memory_space=pltpu.VMEM)
        dma = pltpu.SemaphoreType.DMA

        meta = jnp.concatenate([route_idx.T.astype(F32) + 1.0, gate_weights.T], axis=1)
        meta = jnp.pad(meta, ((0, 8 - top_k), (0, 0)))

        xs, gates, counts = pl.pallas_call(
            functools.partial(dispatch_kernel, tok, cap, win),
            out_shape=(jax.ShapeDtypeStruct((experts, chips, pair_rows, d_model), BF16),
                       jax.ShapeDtypeStruct((ep_size, 3 * tok, experts * win), BF16),
                       jax.ShapeDtypeStruct((experts, 128), jnp.int32)),
            in_specs=[any_space, vmem],
            out_specs=(any_space, any_space, vmem),
            scratch_shapes=[
                pltpu.VMEM((ep_size, tok, d_model), BF16),
                pltpu.VMEM((ep_size, 8, 2 * tok), F32),
                pltpu.VMEM((chips, experts * pair_rows, 2 * tok), BF16),
                pltpu.VMEM((chips, experts, pair_rows, d_model), BF16),
                pltpu.VMEM((ep_size, 3 * tok, experts * win), BF16),
                pltpu.VMEM((2 * tok, 2 * tok), BF16),
                dma((2,)), dma((7,)), dma((7,)),
                dma((tiles + tiles // 2,)), dma((tiles + tiles // 2,)), dma((tiles + tiles // 2,)), dma((tiles + tiles // 2,)),
                dma((4 * tiles,)), dma((4 * tiles,)), dma((chips, tiles)), dma,
            ],
            compiler_params=pltpu.CompilerParams(collective_id=0, has_side_effects=True, vmem_limit_bytes=VMEM_LIMIT),
            name='dispatch',
        )(hidden, meta)

        early = min(EARLY, experts)
        late = experts - early
        held = max(late, 1)
        outs, act = pl.pallas_call(
            functools.partial(ffn_kernel, cap, early),
            out_shape=(jax.ShapeDtypeStruct(xs.shape, BF16),
                       jax.ShapeDtypeStruct((held, chips, pair_rows, d_ff), BF16)),
            in_specs=[pl.BlockSpec(memory_space=pltpu.SMEM)] + [any_space] * 4,
            out_specs=(any_space, any_space),
            scratch_shapes=[
                pltpu.VMEM((3, rows, d_model), BF16),
                pltpu.VMEM((W_SLOTS, d_model, FCOL), BF16),
                pltpu.VMEM((W_SLOTS, d_model, FCOL), BF16),
                pltpu.VMEM((DN_SLOTS, d_ff, FCOL), BF16),
                pltpu.VMEM((2, rows, d_ff), BF16),
                pltpu.VMEM((CHUNK, d_ff), BF16),
                dma((3, rows // CHUNK)), dma((W_SLOTS, 2)), dma((DN_SLOTS,)), dma((2, chips, pair_rows // CHUNK)),
            ],
            input_output_aliases={1: 0},
            compiler_params=pltpu.CompilerParams(vmem_limit_bytes=VMEM_LIMIT),
            name='experts',
        )(counts, xs, w_gate, w_up, w_down)

        return pl.pallas_call(
            functools.partial(combine_kernel, tok, win, early),
            out_shape=jax.ShapeDtypeStruct((tok, d_model), BF16),
            in_specs=[any_space] * 4,
            out_specs=vmem,
            scratch_shapes=[
                pltpu.VMEM((held, rows, d_ff), BF16),
                pltpu.VMEM((ep_size, 3 * tok, experts * win), BF16),
                pltpu.VMEM((D_SLOTS, d_ff, WIDE), BF16),
                pltpu.VMEM((2, ep_size, experts, win, WIDE), BF16),
                pltpu.VMEM((2, chips, halves, tok, COL), F32),
                pltpu.VMEM((Z_SLOTS, chips, halves, tok, COL), F32),
                pltpu.VMEM((blocks, chips, halves, tok, COL), F32),
                pltpu.VMEM((blocks, 2 * halves, tok // 2, COL), F32),
                pltpu.VMEM((blocks, 2 * halves, tok, COL), F32),
                dma((held,)), dma, dma((D_SLOTS,)), dma((2, ep_size)),
                dma((2, chips)), dma((blocks, chips)),
                dma((blocks, 2 * halves)), dma((blocks, 2 * halves)), dma((blocks, 2 * halves)), dma((blocks, 2 * halves)),
            ],
            compiler_params=pltpu.CompilerParams(collective_id=1, has_side_effects=True, vmem_limit_bytes=VMEM_LIMIT),
            name='down_combine',
        )(outs, act.reshape(held, rows, d_ff), gates, w_down)

    row_spec = P(('dp', 'ep'), None)
    expert_spec = P('ep', None, None)
    return jax.shard_map(device_body, mesh=mesh, in_specs=(row_spec, row_spec, row_spec, expert_spec, expert_spec, expert_spec), out_specs=row_spec, check_vma=False)
```
